128 devices in a mesh: row: 4 (over z), col: 2 (over y_lo), ex: 16 (over x, y_hi, core).
Axes of the slice: x: 4, y: 4 (y_hi: 2, y_lo: 2; y = y_hi * 2 + y_lo), z: 4, core: 2. Of those that a mesh axis runs over, the one named last changes fastest.
Arguments:
- train_in: bfloat16 [8192, 8192], P('ex', 'row'), may hold values from -6 to 6
- train_out: bfloat16 [8192, 8192], P('ex', 'col'), may hold values from -0.0047912598 to 0.0047912598
- query_in: bfloat16 [512, 8192], P('ex', 'row'), may hold values from -6 to 6
- query_out: bfloat16 [512, 8192], P('ex', 'col'), may hold values from -0.023925781 to 0.023925781
- query_ids: int32 [512], P('ex'), may hold values from 0 to 1
- in_basis: bfloat16 [8, 1024, 1024], P('row'), may hold values from -1 to 1, as said below
- out_basis: bfloat16 [8, 1024, 1024], P('col'), may hold values from -1 to 1, as said below
- level_table: float32 [64, 64], replicated, may hold values from 0.5 to 8
- in_level: int32 [8192], P('row'), may hold values from 0 to 63
- out_level: int32 [8192], P('col'), may hold values from 0 to 63
- lengths: int32 [4], replicated, may hold values from 1 to 4096, 8192 in all
Outputs:
- token_scores: float32 [2, 8192], P(None, 'ex')
- example_scores: float32 [2, 4], replicated
The draws below stay inside these ranges and needn't reach their ends.
Inputs may be any that keep to these rules, and one draw needn't show every extreme that they name: `in_basis`: each block is an orthogonal matrix rounded to bfloat16. `out_basis`: each block is an orthogonal matrix rounded to bfloat16. `lengths`: the counts sum to 8192.
All inputs are finite; a program needn't handle non-finite values.
Results may differ from the reference program's by a relative error of at most 0.018.
Values may be sent and summed in bfloat16 or wider, within the bound.
No kernel may reach another device: no remote copies, remote signals or barrier semaphores. Data moves between devices by JAX's collectives and lax.ppermute only.
A program may use at most 192 MiB of HBM per device.

```python
import math
import jax
import jax.numpy as jnp
import numpy as np
from jax import lax

D_IN = 8192
D_OUT = 8192
BLOCK = 1024
QUERIES = 2
LEVELS = 64
EXAMPLES = 4
TOKENS = 8192
QTOKENS = 512
MOSTLEN = 4096
IN_BLOCKS = 8
OUT_BLOCKS = 8


def orthogonal_blocks(key, count):
    normal = jax.random.normal(key, (count, BLOCK, BLOCK), jnp.float32)
    factor, upper = jnp.linalg.qr(normal)
    return factor


def draw_in_basis(key, part):
    return orthogonal_blocks(jax.random.fold_in(key, 11), IN_BLOCKS).astype(jnp.bfloat16)


def draw_out_basis(key, part):
    return orthogonal_blocks(jax.random.fold_in(key, 23), OUT_BLOCKS).astype(jnp.bfloat16)


def place_ends(result, own_key, smallest, high):
    dims = result.shape
    index_at = [jax.random.randint(jax.random.fold_in(own_key, axis), (), 0, dims[axis]) for axis in range(len(dims))]
    result = result.at[tuple(index_at)].set(smallest)
    longest = dims.index(max(dims))
    index_at[longest] = (index_at[longest] + 1) % dims[longest]
    return result.at[tuple(index_at)].set(high)


def levels(rng, shape, cuts, least, top_value):
    factor_of = 1.0
    for axis_at, parts in cuts:
        heights = jax.random.uniform(jax.random.fold_in(jax.random.fold_in(rng, 6), axis_at), (parts,), jnp.float32, least / len(cuts), top_value / len(cuts))
        factor_of = factor_of * jnp.repeat(jnp.exp(heights), shape[axis_at] // parts).reshape((-1,) + (1,) * (len(shape) - 1 - axis_at))
    return factor_of


def split_up(amount, total, bound, lean):
    weights = [(1 << 20) // math.isqrt(standing ** lean) + 1 for standing in range(2, amount + 1)]
    surplus, given = total - bound - (amount - 1), [1] * (amount - 1)
    while surplus > 0:
        movable = [i for i in range(amount - 1) if given[i] < bound]
        whole, remaining = sum([weights[i] for i in movable]), surplus
        for i in movable:
            extra = min(bound - given[i], max(1, remaining * weights[i] // whole), surplus)
            given[i] = given[i] + extra
            surplus = surplus - extra
    return np.array([bound] + given)


def uneven(own_key, number_of, total, bound, slope):
    if number_of == 2:
        one = jax.random.randint(own_key, (), max(1, total - bound), min(bound, total - 1) + 1)
        return jnp.stack([one, total - one])
    tallies = jnp.asarray(split_up(number_of, total, bound, slope), jnp.int32)
    pairs = (number_of - 1) // 2
    source_of, sink = tallies[1:1 + 2 * pairs:2], tallies[2:2 + 2 * pairs:2]
    room = jnp.minimum(source_of - 1, bound - sink)
    shifted = jax.random.randint(jax.random.fold_in(own_key, 1), (pairs,), 0, 1 << 20) % (room + 1)
    tallies = tallies.at[1:1 + 2 * pairs:2].set(source_of - shifted).at[2:2 + 2 * pairs:2].set(sink + shifted)
    return tallies[jax.random.permutation(jax.random.fold_in(own_key, 2), number_of)]


def gaussian(own_key, dims, spread, limit, pieces=(), kind=jnp.bfloat16):
    values = jax.random.normal(own_key, dims, jnp.float32) * spread
    if len(pieces) > 0:
        values = levels(own_key, dims, pieces, -0.22, 0.18) * values
    return jnp.clip(values, min=-limit, max=limit).astype(kind)


def setup_inputs(seed: int = 0) -> dict:
    splits = jax.random.split(jax.random.key(seed), 12)
    return {
        "train_in": gaussian(splits[0], (TOKENS, D_IN), 1.0, 6.0, ((0, 16), (1, 4))),
        "train_out": gaussian(splits[1], (TOKENS, D_OUT), 0.0008, 0.0047912598, ((0, 16), (1, 2))),
        "query_in": gaussian(splits[2], (QTOKENS, D_IN), 1.0, 6.0, ((0, 16), (1, 4))),
        "query_out": gaussian(splits[3], (QTOKENS, D_OUT), 0.004, 0.023925781, ((0, 16), (1, 2))),
        "query_ids": place_ends(jax.random.randint(splits[4], (QTOKENS,), 0, QUERIES), jax.random.fold_in(splits[4], 1), 0, QUERIES - 1).astype(jnp.int32),
        "in_basis": draw_in_basis(jax.random.fold_in(splits[11], 71), 0),
        "out_basis": draw_out_basis(jax.random.fold_in(splits[11], 71), 0),
        "level_table": jnp.clip(jnp.exp(jax.random.uniform(splits[7], (LEVELS, LEVELS), jnp.float32, math.log(0.5), math.log(8.0))), 0.5, 8.0),
        "in_level": place_ends(jax.random.randint(splits[8], (D_IN,), 0, LEVELS), jax.random.fold_in(splits[8], 1), 0, LEVELS - 1).astype(jnp.int32),
        "out_level": place_ends(jax.random.randint(splits[9], (D_OUT,), 0, LEVELS), jax.random.fold_in(splits[9], 1), 0, LEVELS - 1).astype(jnp.int32),
        "lengths": uneven(splits[10], EXAMPLES, TOKENS, MOSTLEN, 2).astype(jnp.int32),
    }


DAMPING = 0.1

def rounded(value):
    return lax.optimization_barrier(value.astype(jnp.bfloat16)).astype(jnp.float32)

def reference(train_in, train_out, query_in, query_out, query_ids, in_basis, out_basis, level_table, in_level, out_level, lengths):
    highest = lax.Precision.HIGHEST
    q_in = query_in.astype(jnp.float32)
    q_out = query_out.astype(jnp.float32)
    basis_out = out_basis.astype(jnp.float32)
    basis_in = in_basis.astype(jnp.float32)
    eigen = level_table[out_level[:, None], in_level[None, :]].reshape(OUT_BLOCKS, BLOCK, IN_BLOCKS, BLOCK)
    acts = train_in.astype(jnp.float32)
    grads = train_out.astype(jnp.float32)

    def per_query(query):
        weights = (query_ids == query).astype(jnp.float32)
        grad = jnp.dot((q_out * weights[:, None]).T, q_in, precision=highest)
        grad = rounded(grad).reshape(OUT_BLOCKS, BLOCK, IN_BLOCKS, BLOCK)
        half = rounded(jnp.einsum('iab,iajc->ibjc', basis_out, grad, precision=highest))
        rotated = jnp.einsum('ibjc,jcd->ibjd', half, basis_in, precision=highest)
        damped = rounded(rotated / (eigen + DAMPING))
        back = rounded(jnp.einsum('ibjd,jcd->ibjc', damped, basis_in, precision=highest))
        precond = rounded(jnp.einsum('iab,ibjc->iajc', basis_out, back, precision=highest))
        precond = precond.reshape(D_OUT, D_IN)
        image = jnp.dot(acts, precond.T, precision=highest)
        return jnp.sum(image * grads, axis=1)
    token_scores = lax.map(per_query, jnp.arange(QUERIES, dtype=jnp.int32))
    ends = jnp.cumsum(lengths).astype(jnp.int32)
    starts = (ends - lengths).astype(jnp.int32)
    positions = jnp.arange(TOKENS, dtype=jnp.int32)
    member = ((positions[None, :] >= starts[:, None]) & (positions[None, :] < ends[:, None])).astype(jnp.float32)
    example_scores = jnp.dot(token_scores, member.T, precision=highest)
    return (token_scores, example_scores)
```

```python
import jax
import jax.numpy as jnp
from jax import lax
from jax.experimental import pallas as pl
from jax.experimental.pallas import tpu as pltpu
from jax.sharding import PartitionSpec as P


QUERIES = 2
DAMPING = 0.1
LANES = 128
BF = jnp.bfloat16
F32 = jnp.float32
UNREAD = pl.BlockSpec(memory_space=pl.ANY)


def vmem_limit(mib):
    return pltpu.CompilerParams(vmem_limit_bytes=mib * 2**20)


def turned_train(train_out, train_in, out_basis, in_basis, core, after=()):
    tokens = train_in.shape[0]
    width = in_basis.shape[1]

    def kernel(core_ref, out_ref, in_ref, outer_ref, inner_ref, *refs):
        away_ref, own_ref, acts_ref = refs[-3:]
        step = pl.program_id(0)

        @pl.when(step < 4)
        def _():
            turned = jnp.dot(out_ref[...], outer_ref[0], preferred_element_type=F32).astype(BF)

            @pl.when(step < 2)
            def _():
                away_ref[0] = turned

            @pl.when(step >= 2)
            def _():
                own_ref[0] = turned

        @pl.when(step >= 4)
        def _():
            acts_ref[0] = jnp.dot(
                in_ref[...], inner_ref[0], preferred_element_type=F32
            ).astype(BF)

    def outer(n, s):
        n = jnp.minimum(n, 3)
        return jnp.where(n < 2, (1 - s[0]) * 2 + n, s[0] * 2 + n - 2)

    def inner(n, s):
        return jnp.where(n < 5, s[0], 1 - s[0])

    def result(first):
        return pl.BlockSpec(
            (1, tokens, width), lambda n, s: (jnp.clip(n - first, 0, 1), 0, 0)
        )

    shape = jax.ShapeDtypeStruct((2, tokens, width), BF)
    return pl.pallas_call(
        kernel,
        grid_spec=pltpu.PrefetchScalarGridSpec(
            num_scalar_prefetch=1,
            grid=(6,),
            in_specs=[
                pl.BlockSpec((tokens, width), lambda n, s: (0, outer(n, s))),
                pl.BlockSpec((tokens, width), lambda n, s: (0, inner(n, s))),
                pl.BlockSpec((1, width, width), lambda n, s: (outer(n, s), 0, 0)),
                pl.BlockSpec((1, width, width), lambda n, s: (inner(n, s), 0, 0)),
            ]
            + [UNREAD] * len(after),
            out_specs=(result(0), result(2), result(4)),
        ),
        out_shape=(shape,) * 3,
        cost_estimate=pl.CostEstimate(
            flops=12 * tokens * width * width,
            bytes_accessed=12 * (2 * tokens * width + width * width),
            transcendentals=0,
        ),
        compiler_params=vmem_limit(60),
        name="turned_train",
    )(core[None], train_out, train_in, out_basis, in_basis, *after)


def level_picks(levels, ref):
    row = lax.broadcasted_iota(jnp.int32, (levels, ref.shape[1]), 0)
    return jnp.where(row == ref[...], 1.0, 0.0).astype(BF)


def inverse_sides(level_table, in_levels, after=()):
    levels = level_table.shape[0]
    inputs = in_levels.shape[1]

    def kernel(table_ref, in_ref, *refs):
        table = 1.0 / (table_ref[...] + DAMPING)
        coarse = table.astype(BF)
        fine = (table - coarse.astype(F32)).astype(BF)
        chosen = level_picks(levels, in_ref)
        for n, part in enumerate((coarse, fine)):
            side = jnp.dot(part, chosen, preferred_element_type=F32)
            refs[-1][:, n * levels : (n + 1) * levels] = side.T.astype(BF)

    vmem = pl.BlockSpec(memory_space=pltpu.VMEM)
    return pl.pallas_call(
        kernel,
        in_specs=[vmem, vmem] + [UNREAD] * len(after),
        out_specs=vmem,
        out_shape=jax.ShapeDtypeStruct((inputs, 2 * levels), BF),
        compiler_params=vmem_limit(16),
        name="inverse_sides",
    )(level_table, in_levels, *after)


def gathered(pieces, split):
    rows, columns = pieces[0].shape
    count = len(pieces)

    def kernel(*refs):
        for n in range(count):
            here = slice(n * rows, (n + 1) * rows)
            refs[count][here] = refs[n][:, :split]
            refs[count + 1][here] = refs[n][:, split:]

    shapes = [(count * rows, w) for w in (split, columns - split)]
    return pl.pallas_call(
        kernel,
        grid=(1,),
        in_specs=[pl.BlockSpec((rows, columns), lambda n: (0, 0))] * count,
        out_specs=[pl.BlockSpec(shape, lambda n: (0, 0)) for shape in shapes],
        out_shape=[jax.ShapeDtypeStruct(shape, BF) for shape in shapes],
        compiler_params=vmem_limit(60),
        name="gathered",
    )(*pieces)


def parcels(query_in, query_out, query_ids, core):
    few, inner = query_in.shape
    outer = query_out.shape[1]
    width, half = inner // 2, outer // 2

    def kernel(core_ref, ids_ref, in_ref, out_ref, keep_ref, send_ref):
        row = lax.broadcasted_iota(jnp.int32, (few, LANES), 0)
        codes = jnp.zeros((few, LANES), F32)
        for n in range(few):
            codes = jnp.where(row == n, ids_ref[n].astype(F32), codes)
        codes = codes.astype(BF)

        def fill(ref, which):
            ref[:, :width] = in_ref[:, which * width : (which + 1) * width]
            ref[:, width : width + half] = out_ref[:, which * half : (which + 1) * half]
            ref[:, width + half :] = codes

        @pl.when(core_ref[0] == 0)
        def _():
            fill(keep_ref, 0)
            fill(send_ref, 1)

        @pl.when(core_ref[0] == 1)
        def _():
            fill(keep_ref, 1)
            fill(send_ref, 0)

    shape = jax.ShapeDtypeStruct((few, width + half + LANES), BF)
    smem = pl.BlockSpec(memory_space=pltpu.SMEM)
    return pl.pallas_call(
        kernel,
        grid=(1,),
        in_specs=[
            smem,
            smem,
            pl.BlockSpec((few, inner), lambda n: (0, 0)),
            pl.BlockSpec((few, outer), lambda n: (0, 0)),
        ],
        out_specs=(pl.BlockSpec(shape.shape, lambda n: (0, 0)),) * 2,
        out_shape=(shape, shape),
        compiler_params=vmem_limit(60),
        name="parcels",
    )(core[None], query_ids, query_in, query_out)


def pooled(kept, got, core, width):
    few, total = kept.shape

    def kernel(core_ref, kept_ref, got_ref, in_ref, outs_ref):
        def fill(ref, at):
            rows = slice(at, at + few)
            in_ref[rows] = ref[:, :width]
            outs_ref[rows, :width] = ref[:, width : 2 * width]
            outs_ref[rows, width : width + LANES] = ref[:, total - LANES :]
            outs_ref[rows, width + LANES :] = ref[:, 2 * width : 3 * width]

        @pl.when(core_ref[0] == 0)
        def _():
            fill(kept_ref, 0)
            fill(got_ref, few)

        @pl.when(core_ref[0] == 1)
        def _():
            fill(got_ref, 0)
            fill(kept_ref, few)

    smem = pl.BlockSpec(memory_space=pltpu.SMEM)
    shapes = [(2 * few, w) for w in (width, total - width)]
    return pl.pallas_call(
        kernel,
        grid=(1,),
        in_specs=[smem] + [pl.BlockSpec((few, total), lambda n: (0, 0))] * 2,
        out_specs=[pl.BlockSpec(shape, lambda n: (0, 0)) for shape in shapes],
        out_shape=[jax.ShapeDtypeStruct(shape, BF) for shape in shapes],
        compiler_params=vmem_limit(60),
        name="pooled",
    )(core[None], kept, got)


def rotate_turned(pieces, basis, which, after=(), strip=1024):
    rows = pieces[0].shape[0]
    width = basis.shape[1]
    count = len(pieces)

    def kernel(start_ref, *refs):
        basis_ref, out_ref = refs[count], refs[-1]
        for n in range(count):
            turned = jnp.dot(refs[n][...], basis_ref[0], preferred_element_type=F32)
            out_ref[:, n * rows : (n + 1) * rows] = turned.T.astype(BF)

    return pl.pallas_call(
        kernel,
        grid_spec=pltpu.PrefetchScalarGridSpec(
            num_scalar_prefetch=1,
            grid=(width // strip,),
            in_specs=[pl.BlockSpec((rows, width), lambda n, s: (0, 0))] * count
            + [pl.BlockSpec((1, width, strip), lambda n, s: (0, 0, n))]
            + [UNREAD] * len(after),
            out_specs=pl.BlockSpec((strip, rows * count), lambda n, s: (n, 0)),
        ),
        out_shape=jax.ShapeDtypeStruct((width, rows * count), BF),
        cost_estimate=pl.CostEstimate(
            flops=2 * count * rows * width * width,
            bytes_accessed=2 * (2 * count * rows * width + width * width),
            transcendentals=0,
        ),
        compiler_params=vmem_limit(20),
        name="rotate_turned",
    )(which[None], *pieces, basis, *after)


def spread_out(pieces, coded, basis, which, unit, after=()):
    width = basis.shape[1]
    count, rows = len(pieces), pieces[0].shape[0]
    operands = list(pieces) + ([] if pieces is coded else list(coded))

    def kernel(start_ref, *refs):
        basis_ref, out_ref = refs[len(operands)], refs[-1]
        for y in range(count):
            turned = jnp.dot(refs[y][:, :width], basis_ref[0], preferred_element_type=F32)
            codes = refs[y if pieces is coded else count + y]
            for x in range(rows // unit):
                here = slice(x * unit, (x + 1) * unit)
                code = codes[here, width : width + 1].astype(F32)
                at = (x * count + y) * unit
                for q in range(QUERIES):
                    out_ref[q, at : at + unit] = jnp.where(
                        code == float(q), turned[here], 0.0
                    ).astype(BF)

    return pl.pallas_call(
        kernel,
        grid_spec=pltpu.PrefetchScalarGridSpec(
            num_scalar_prefetch=1,
            grid=(1,),
            in_specs=[pl.BlockSpec(p.shape, lambda n, s: (0, 0)) for p in operands]
            + [pl.BlockSpec((1, width, width), lambda n, s: (0, 0, 0))]
            + [UNREAD] * len(after),
            out_specs=pl.BlockSpec((QUERIES, count * rows, width), lambda n, s: (0, 0, 0)),
        ),
        out_shape=jax.ShapeDtypeStruct((QUERIES, count * rows, width), BF),
        cost_estimate=pl.CostEstimate(
            flops=2 * count * rows * width * width,
            bytes_accessed=2 * (3 * count * rows * width + width * width),
            transcendentals=0,
        ),
        compiler_params=vmem_limit(20),
        name="spread_out",
    )(which[None], *operands, basis, *after)


def score_block(
    turned, spread, sides, out_levels, acts, grads, running, block, strip=512, rows=256
):
    width, qtokens = turned[0].shape
    parts, tokens = acts[0].shape[:2]
    total_shape = (QUERIES, 2 * tokens, LANES)
    strips = width // strip

    levels = sides.shape[1] // 2

    def kernel(t0, t1, spread_ref, sides_ref, levels_ref, a0, a1, g0, g1, *refs):
        out_ref, scratch, inverse_ref = refs[-3:]

        @pl.when(pl.program_id(0) == 0)
        def _():
            out_ref[...] = jnp.zeros(total_shape, F32) if running is None else refs[0][...]

        chosen = level_picks(levels, levels_ref)
        chosen = jnp.concatenate([chosen, chosen])
        for top in range(0, parts * width, rows):
            at = slice(top, top + rows)
            inverse_ref[at] = jnp.dot(sides_ref[at], chosen, preferred_element_type=F32)

        for q in range(QUERIES):
            for p, t in enumerate((t0, t1)):
                for top in range(0, width, rows):
                    at = slice(p * width + top, p * width + top + rows)
                    piece = jnp.dot(t[top : top + rows], spread_ref[q], preferred_element_type=F32)
                    scratch[at] = (piece * inverse_ref[at]).astype(BF)
            for side, (a, g) in enumerate(((a0, g0), (a1, g1))):
                for top in range(0, tokens, rows):
                    image = None
                    for p in range(parts):
                        term = jnp.dot(
                            a[p if side == 0 else 1 - p, top : top + rows],
                            scratch[p * width : (p + 1) * width],
                            preferred_element_type=F32,
                        )
                        image = term if image is None else image + term
                    terms = image * g[0, top : top + rows].astype(F32)
                    total = terms[:, :LANES]
                    for lane in range(LANES, strip, LANES):
                        total = total + terms[:, lane : lane + LANES]
                    at = side * tokens + top
                    out_ref[q, at : at + rows] += total

    once = pl.Buffered(1)
    whole = pl.BlockSpec(acts[0].shape, lambda n: (0, 0, 0), pipeline_mode=once)
    turned_spec = pl.BlockSpec((width, qtokens), lambda n: (0, 0), pipeline_mode=once)
    strip_spec = pl.BlockSpec((1, tokens, strip), lambda n: (block, 0, n))
    run_spec = pl.BlockSpec(total_shape, lambda n: (0, 0, 0), pipeline_mode=once)
    flops = 2 * QUERIES * parts * width * width * (qtokens + 2 * tokens)
    return pl.pallas_call(
        kernel,
        grid=(strips,),
        in_specs=[
            turned_spec,
            turned_spec,
            pl.BlockSpec((QUERIES, qtokens, strip), lambda n: (0, 0, n)),
            pl.BlockSpec(sides.shape, lambda n: (0, 0), pipeline_mode=once),
            pl.BlockSpec((1, strip), lambda n: (0, block * strips + n)),
            whole,
            whole,
            strip_spec,
            strip_spec,
        ]
        + ([] if running is None else [run_spec]),
        out_specs=pl.BlockSpec(total_shape, lambda n: (0, 0, 0)),
        out_shape=jax.ShapeDtypeStruct(total_shape, F32),
        scratch_shapes=[
            pltpu.VMEM((parts * width, strip), BF),
            pltpu.VMEM((parts * width, strip), F32),
        ],
        cost_estimate=pl.CostEstimate(flops=flops, bytes_accessed=16 * 2**20, transcendentals=0),
        compiler_params=vmem_limit(32),
        name="score_block",
    )(*turned, spread, sides, out_levels, *acts, *grads, *([] if running is None else [running]))


def body(
    train_in,
    train_out,
    query_in,
    query_out,
    query_ids,
    in_basis,
    out_basis,
    level_table,
    in_level,
    out_level,
    lengths,
):
    ex_count = lax.axis_size("ex")
    ex_index = lax.axis_index("ex")
    core = ex_index % 2
    in_sub, width = in_basis.shape[0], in_basis.shape[1]
    out_sub = out_basis.shape[0]
    half = out_sub // 2
    tokens = train_in.shape[0]
    few = query_in.shape[0]
    hops = ex_count // 4

    def to_core(a):
        return lax.ppermute(a, "ex", [(i, i ^ 1) for i in range(ex_count)])

    def across_y(a):
        return lax.ppermute(a, "ex", [(i, i ^ 2) for i in range(ex_count)])

    def across_y_and_col(a):
        count = lax.axis_size("col") * ex_count
        return lax.ppermute(a, ("col", "ex"), [(i, i ^ ex_count ^ 2) for i in range(count)])

    def along_x(a):
        return [a] + [
            lax.ppermute(a, "ex", [(i, (i + 4 * n) % ex_count) for i in range(ex_count)])
            for n in range(1, hops)
        ]

    kept, sent = parcels(query_in, query_out, query_ids, core)
    near_in, near_out = pooled(kept, to_core(sent), core, width)
    near_in_y = across_y_and_col(near_in)
    column = jnp.concatenate([near_in, near_in_y])
    row = along_x(near_out)
    rows = gathered(row, width + LANES)
    grads_away, grads_own, acts_own = turned_train(
        train_out, train_in, out_basis, in_basis, core, (near_in,)
    )
    first_pieces, second_pieces = ([r, across_y(r)] for r in rows)
    in_pieces = along_x(column)
    grads_other = to_core(grads_away)
    acts_other = to_core(acts_own)

    in_levels = in_level.reshape(in_sub, width)
    in_levels = jnp.concatenate(
        [lax.dynamic_slice_in_dim(in_levels, n, 1) for n in (core, 1 - core)], axis=1
    )
    out_levels = lax.dynamic_slice_in_dim(out_level, core * half * width, half * width)[None]
    sides = inverse_sides(level_table, in_levels, (grads_own,))

    inner = lax.dynamic_slice_in_dim(in_basis, core, 1)
    outers = [lax.dynamic_slice_in_dim(out_basis, core * half + n, 1) for n in range(half)]
    query_own = rotate_turned(in_pieces, inner, core, (sides, first_pieces[1]))
    query_other = to_core(query_own)
    running = None
    for block, pieces in enumerate((first_pieces, second_pieces)):
        spread = spread_out(
            pieces,
            first_pieces,
            outers[block],
            core,
            2 * few,
            () if running is None else (running,),
        )
        running = score_block(
            (query_own, query_other),
            spread,
            sides,
            out_levels,
            (acts_own, acts_other),
            (grads_own, grads_other),
            running,
            block,
        )

    part = jnp.sum(running, axis=2)
    mine, others = part[:, :tokens], part[:, tokens:]
    token_part = mine + to_core(others)

    def sum_over(shard, axes):
        size = lax.axis_size(axes)
        spread = jnp.broadcast_to(shard[None], (size, *shard.shape))
        return jnp.sum(lax.all_to_all(spread, axes, 0, 0, tiled=True), axis=0)

    token_scores = sum_over(token_part, ("row", "col"))
    ends = jnp.cumsum(lengths)
    starts = ends - lengths
    at = ex_index * tokens + jnp.arange(tokens, dtype=jnp.int32)
    member = (at[None, :] >= starts[:, None]) & (at[None, :] < ends[:, None])
    example_part = jnp.sum(jnp.where(member[None], token_scores[:, None, :], 0.0), axis=2)
    example_scores = sum_over(example_part, "ex")
    return (token_scores, example_scores)


def solution(mesh):
    placed = (
        P("ex", "row"),
        P("ex", "col"),
        P("ex", "row"),
        P("ex", "col"),
        P("ex"),
        P("row", None, None),
        P("col", None, None),
        P(),
        P("row"),
        P("col"),
        P(),
    )
    return jax.shard_map(
        body, mesh=mesh, in_specs=placed, out_specs=(P(None, "ex"), P()), check_vma=False
    )
```

```python
import jax
import jax.numpy as jnp
from jax import lax
from jax.experimental import pallas as pl
from jax.experimental.pallas import tpu as pltpu
from jax.sharding import PartitionSpec as P


QUERIES = 2
DAMPING = 0.1
LANES = 128
BF = jnp.bfloat16
F32 = jnp.float32
UNREAD = pl.BlockSpec(memory_space=pl.ANY)


def vmem_limit(mib):
    return pltpu.CompilerParams(vmem_limit_bytes=mib * 2**20)


def turned_pairs(tokens, basis, pick, groups, kept, core, after=()):
    rows = tokens.shape[0]
    width = basis.shape[1]

    def kernel(core_ref, tokens_ref, basis_ref, *refs):
        step = pl.program_id(0)
        turned = jnp.dot(tokens_ref[...], basis_ref[0], preferred_element_type=F32).astype(BF)
        for group in range(groups):

            @pl.when(step // 2 == group)
            def _(group=group):
                refs[len(after) + group][0] = turned

        for n, when in enumerate(kept):

            @pl.when(step == when)
            def _(n=n):
                refs[len(after) + groups + n][...] = basis_ref[...]

    def result(group):
        return pl.BlockSpec(
            (1, rows, width), lambda n, s: (jnp.clip(n - 2 * group, 0, 1), 0, 0)
        )

    shape = jax.ShapeDtypeStruct((2, rows, width), BF)
    return pl.pallas_call(
        kernel,
        grid_spec=pltpu.PrefetchScalarGridSpec(
            num_scalar_prefetch=1,
            grid=(2 * groups,),
            in_specs=[
                pl.BlockSpec((rows, width), lambda n, s: (0, pick(n, s[0]))),
                pl.BlockSpec((1, width, width), lambda n, s: (pick(n, s[0]), 0, 0)),
            ]
            + [UNREAD] * len(after),
            out_specs=[result(group) for group in range(groups)]
            + [pl.BlockSpec((1, width, width), lambda n, s: (0, 0, 0))] * len(kept),
        ),
        out_shape=[shape] * groups
        + [jax.ShapeDtypeStruct((1, width, width), BF)] * len(kept),
        cost_estimate=pl.CostEstimate(
            flops=4 * groups * rows * width * width,
            bytes_accessed=4 * groups * (2 * rows * width + width * width),
            transcendentals=0,
        ),
        compiler_params=vmem_limit(50),
        name="turned_pairs",
    )(core[None], tokens, basis, *after)


def level_picks(levels, ref):
    row = lax.broadcasted_iota(jnp.int32, (levels, ref.shape[1]), 0)
    return jnp.where(row == ref[...], 1.0, 0.0).astype(BF)


def inverse_sides(level_table, in_levels, after=()):
    levels = level_table.shape[0]
    inputs = in_levels.shape[1]

    def kernel(table_ref, in_ref, *refs):
        table = 1.0 / (table_ref[...] + DAMPING)
        coarse = table.astype(BF)
        fine = (table - coarse.astype(F32)).astype(BF)
        chosen = level_picks(levels, in_ref)
        for n, part in enumerate((coarse, fine)):
            side = jnp.dot(part, chosen, preferred_element_type=F32)
            refs[-1][:, n * levels : (n + 1) * levels] = side.T.astype(BF)

    vmem = pl.BlockSpec(memory_space=pltpu.VMEM)
    return pl.pallas_call(
        kernel,
        in_specs=[vmem, vmem] + [UNREAD] * len(after),
        out_specs=vmem,
        out_shape=jax.ShapeDtypeStruct((inputs, 2 * levels), BF),
        compiler_params=vmem_limit(16),
        name="inverse_sides",
    )(level_table, in_levels, *after)


def gathered(pieces, split):
    rows, columns = pieces[0].shape
    count = len(pieces)

    def kernel(*refs):
        for n in range(count):
            here = slice(n * rows, (n + 1) * rows)
            refs[count][here] = refs[n][:, :split]
            refs[count + 1][here] = refs[n][:, split:]

    shapes = [(count * rows, w) for w in (split, columns - split)]
    return pl.pallas_call(
        kernel,
        grid=(1,),
        in_specs=[pl.BlockSpec((rows, columns), lambda n: (0, 0))] * count,
        out_specs=[pl.BlockSpec(shape, lambda n: (0, 0)) for shape in shapes],
        out_shape=[jax.ShapeDtypeStruct(shape, BF) for shape in shapes],
        compiler_params=vmem_limit(8),
        name="gathered",
    )(*pieces)


def parcels(query_in, query_out, query_ids, core):
    few, inner = query_in.shape
    outer = query_out.shape[1]
    width, half = inner // 2, outer // 2

    def kernel(core_ref, ids_ref, in_ref, out_ref, keep_ref, send_ref):
        row = lax.broadcasted_iota(jnp.int32, (few, LANES), 0)
        codes = jnp.zeros((few, LANES), F32)
        for n in range(few):
            codes = jnp.where(row == n, ids_ref[n].astype(F32), codes)
        codes = codes.astype(BF)

        def fill(ref, which):
            ref[:, :width] = in_ref[:, which * width : (which + 1) * width]
            ref[:, width : width + half] = out_ref[:, which * half : (which + 1) * half]
            ref[:, width + half :] = codes

        @pl.when(core_ref[0] == 0)
        def _():
            fill(keep_ref, 0)
            fill(send_ref, 1)

        @pl.when(core_ref[0] == 1)
        def _():
            fill(keep_ref, 1)
            fill(send_ref, 0)

    shape = jax.ShapeDtypeStruct((few, width + half + LANES), BF)
    smem = pl.BlockSpec(memory_space=pltpu.SMEM)
    return pl.pallas_call(
        kernel,
        grid=(1,),
        in_specs=[
            smem,
            smem,
            pl.BlockSpec((few, inner), lambda n: (0, 0)),
            pl.BlockSpec((few, outer), lambda n: (0, 0)),
        ],
        out_specs=(pl.BlockSpec(shape.shape, lambda n: (0, 0)),) * 2,
        out_shape=(shape, shape),
        compiler_params=vmem_limit(60),
        name="parcels",
    )(core[None], query_ids, query_in, query_out)


def pooled(kept, got, core, width):
    few, total = kept.shape

    def kernel(core_ref, kept_ref, got_ref, in_ref, outs_ref):
        def fill(ref, at):
            rows = slice(at, at + few)
            in_ref[rows] = ref[:, :width]
            outs_ref[rows, :width] = ref[:, width : 2 * width]
            outs_ref[rows, width : width + LANES] = ref[:, total - LANES :]
            outs_ref[rows, width + LANES :] = ref[:, 2 * width : 3 * width]

        @pl.when(core_ref[0] == 0)
        def _():
            fill(kept_ref, 0)
            fill(got_ref, few)

        @pl.when(core_ref[0] == 1)
        def _():
            fill(got_ref, 0)
            fill(kept_ref, few)

    smem = pl.BlockSpec(memory_space=pltpu.SMEM)
    shapes = [(2 * few, w) for w in (width, total - width)]
    return pl.pallas_call(
        kernel,
        grid=(1,),
        in_specs=[smem] + [pl.BlockSpec((few, total), lambda n: (0, 0))] * 2,
        out_specs=[pl.BlockSpec(shape, lambda n: (0, 0)) for shape in shapes],
        out_shape=[jax.ShapeDtypeStruct(shape, BF) for shape in shapes],
        compiler_params=vmem_limit(8),
        name="pooled",
    )(core[None], kept, got)


def rotate_turned(pieces, basis, which, after=(), strip=1024):
    rows = pieces[0].shape[0]
    width = basis.shape[1]
    count = len(pieces)

    def kernel(start_ref, *refs):
        basis_ref, out_ref = refs[count], refs[-1]
        for n in range(count):
            turned = jnp.dot(refs[n][...], basis_ref[0], preferred_element_type=F32)
            out_ref[:, n * rows : (n + 1) * rows] = turned.T.astype(BF)

    return pl.pallas_call(
        kernel,
        grid_spec=pltpu.PrefetchScalarGridSpec(
            num_scalar_prefetch=1,
            grid=(width // strip,),
            in_specs=[pl.BlockSpec((rows, width), lambda n, s: (0, 0))] * count
            + [pl.BlockSpec((1, width, strip), lambda n, s: (0, 0, n))]
            + [UNREAD] * len(after),
            out_specs=pl.BlockSpec((strip, rows * count), lambda n, s: (n, 0)),
        ),
        out_shape=jax.ShapeDtypeStruct((width, rows * count), BF),
        cost_estimate=pl.CostEstimate(
            flops=2 * count * rows * width * width,
            bytes_accessed=2 * (2 * count * rows * width + width * width),
            transcendentals=0,
        ),
        compiler_params=vmem_limit(60),
        name="rotate_turned",
    )(which[None], *pieces, basis, *after)


def spread_out(pieces, coded, basis, which, unit, after=()):
    width = basis.shape[1]
    count, rows = len(pieces), pieces[0].shape[0]
    operands = list(pieces) + ([] if pieces is coded else list(coded))

    def kernel(start_ref, *refs):
        basis_ref, out_ref = refs[len(operands)], refs[-1]
        for y in range(count):
            turned = jnp.dot(refs[y][:, :width], basis_ref[0], preferred_element_type=F32)
            codes = refs[y if pieces is coded else count + y]
            for x in range(rows // unit):
                here = slice(x * unit, (x + 1) * unit)
                code = codes[here, width : width + 1].astype(F32)
                at = (x * count + y) * unit
                for q in range(QUERIES):
                    out_ref[q, at : at + unit] = jnp.where(
                        code == float(q), turned[here], 0.0
                    ).astype(BF)

    return pl.pallas_call(
        kernel,
        grid_spec=pltpu.PrefetchScalarGridSpec(
            num_scalar_prefetch=1,
            grid=(1,),
            in_specs=[pl.BlockSpec(p.shape, lambda n, s: (0, 0)) for p in operands]
            + [pl.BlockSpec((1, width, width), lambda n, s: (0, 0, 0))]
            + [UNREAD] * len(after),
            out_specs=pl.BlockSpec((QUERIES, count * rows, width), lambda n, s: (0, 0, 0)),
        ),
        out_shape=jax.ShapeDtypeStruct((QUERIES, count * rows, width), BF),
        cost_estimate=pl.CostEstimate(
            flops=2 * count * rows * width * width,
            bytes_accessed=2 * (3 * count * rows * width + width * width),
            transcendentals=0,
        ),
        compiler_params=vmem_limit(20),
        name="spread_out",
    )(which[None], *operands, basis, *after)


def score_block(
    turned, spread, sides, out_levels, acts, grads, running, block, strip=512, rows=256
):
    width, qtokens = turned[0].shape
    parts, tokens = acts[0].shape[:2]
    total_shape = (QUERIES, 2 * tokens, LANES)
    strips = width // strip

    levels = sides.shape[1] // 2

    def kernel(t0, t1, spread_ref, sides_ref, levels_ref, a0, a1, g0, g1, *refs):
        out_ref, scratch, inverse_ref = refs[-3:]

        @pl.when(pl.program_id(0) == 0)
        def _():
            out_ref[...] = jnp.zeros(total_shape, F32) if running is None else refs[0][...]

        chosen = level_picks(levels, levels_ref)
        chosen = jnp.concatenate([chosen, chosen])
        for top in range(0, parts * width, rows):
            at = slice(top, top + rows)
            inverse_ref[at] = jnp.dot(sides_ref[at], chosen, preferred_element_type=F32)

        for q in range(QUERIES):
            for p, t in enumerate((t0, t1)):
                for top in range(0, width, rows):
                    at = slice(p * width + top, p * width + top + rows)
                    piece = jnp.dot(t[top : top + rows], spread_ref[q], preferred_element_type=F32)
                    scratch[at] = (piece * inverse_ref[at]).astype(BF)
            for side, (a, g) in enumerate(((a0, g0), (a1, g1))):
                for top in range(0, tokens, rows):
                    image = None
                    for p in range(parts):
                        term = jnp.dot(
                            a[p if side == 0 else 1 - p, top : top + rows],
                            scratch[p * width : (p + 1) * width],
                            preferred_element_type=F32,
                        )
                        image = term if image is None else image + term
                    terms = image * g[0, top : top + rows].astype(F32)
                    total = terms[:, :LANES]
                    for lane in range(LANES, strip, LANES):
                        total = total + terms[:, lane : lane + LANES]
                    at = side * tokens + top
                    out_ref[q, at : at + rows] += total

    once = pl.Buffered(1)
    whole = pl.BlockSpec(acts[0].shape, lambda n: (0, 0, 0), pipeline_mode=once)
    turned_spec = pl.BlockSpec((width, qtokens), lambda n: (0, 0), pipeline_mode=once)
    strip_spec = pl.BlockSpec((1, tokens, strip), lambda n: (block, 0, n))
    run_spec = pl.BlockSpec(total_shape, lambda n: (0, 0, 0), pipeline_mode=once)
    flops = 2 * QUERIES * parts * width * width * (qtokens + 2 * tokens)
    return pl.pallas_call(
        kernel,
        grid=(strips,),
        in_specs=[
            turned_spec,
            turned_spec,
            pl.BlockSpec((QUERIES, qtokens, strip), lambda n: (0, 0, n)),
            pl.BlockSpec(sides.shape, lambda n: (0, 0), pipeline_mode=once),
            pl.BlockSpec((1, strip), lambda n: (0, block * strips + n)),
            whole,
            whole,
            strip_spec,
            strip_spec,
        ]
        + ([] if running is None else [run_spec]),
        out_specs=pl.BlockSpec(total_shape, lambda n: (0, 0, 0)),
        out_shape=jax.ShapeDtypeStruct(total_shape, F32),
        scratch_shapes=[
            pltpu.VMEM((parts * width, strip), BF),
            pltpu.VMEM((parts * width, strip), F32),
        ],
        cost_estimate=pl.CostEstimate(flops=flops, bytes_accessed=16 * 2**20, transcendentals=0),
        compiler_params=vmem_limit(32),
        name="score_block",
    )(*turned, spread, sides, out_levels, *acts, *grads, *([] if running is None else [running]))


def body(
    train_in,
    train_out,
    query_in,
    query_out,
    query_ids,
    in_basis,
    out_basis,
    level_table,
    in_level,
    out_level,
    lengths,
):
    ex_count = lax.axis_size("ex")
    ex_index = lax.axis_index("ex")
    core = ex_index % 2
    in_sub, width = in_basis.shape[0], in_basis.shape[1]
    out_sub = out_basis.shape[0]
    half = out_sub // 2
    tokens = train_in.shape[0]
    few = query_in.shape[0]
    hops = ex_count // 4

    def to_core(a):
        return lax.ppermute(a, "ex", [(i, i ^ 1) for i in range(ex_count)])

    def across_y(a):
        return lax.ppermute(a, "ex", [(i, i ^ 2) for i in range(ex_count)])

    def across_y_and_col(a):
        count = lax.axis_size("col") * ex_count
        return lax.ppermute(a, ("col", "ex"), [(i, i ^ ex_count ^ 2) for i in range(count)])

    def along_x(a):
        result = [a]
        for n in range(1, hops):
            pairs = [(i, (i + 4 * n) % ex_count) for i in range(ex_count)]
            result.append(lax.ppermute(a, "ex", pairs))
        return result

    kept, sent = parcels(query_in, query_out, query_ids, core)
    near_in, near_out = pooled(kept, to_core(sent), core, width)
    near_in_y = across_y_and_col(near_in)
    column = jnp.concatenate([near_in, near_in_y])
    row = along_x(near_out)
    rows = gathered(row, width + LANES)
    grads_away, grads_own, *outers = turned_pairs(
        train_out,
        out_basis,
        lambda n, c: jnp.where(n < 2, (1 - c) * 2 + n, c * 2 + n - 2),
        2,
        (2, 3),
        core,
        (near_in,),
    )
    grads_other = to_core(grads_away)
    in_pieces = along_x(column)
    first_pieces = [rows[0], across_y(rows[0])]
    second_pieces = [rows[1], across_y(rows[1])]
    acts_own, inner = turned_pairs(
        train_in,
        in_basis,
        lambda n, c: jnp.where(n < 1, c, 1 - c),
        1,
        (0,),
        core,
        (column, *rows),
    )
    acts_other = to_core(acts_own)

    in_levels = in_level.reshape(in_sub, width)
    in_levels = jnp.concatenate(
        [lax.dynamic_slice_in_dim(in_levels, n, 1) for n in (core, 1 - core)], axis=1
    )
    out_levels = lax.dynamic_slice_in_dim(out_level, core * half * width, half * width)[None]
    sides = inverse_sides(level_table, in_levels)

    query_own = rotate_turned(in_pieces, inner, core)
    query_other = to_core(query_own)
    running = None
    for block, pieces in enumerate((first_pieces, second_pieces)):
        spread = spread_out(
            pieces,
            first_pieces,
            outers[block],
            core,
            2 * few,
            () if running is None else (running,),
        )
        running = score_block(
            (query_own, query_other),
            spread,
            sides,
            out_levels,
            (acts_own, acts_other),
            (grads_own, grads_other),
            running,
            block,
        )

    def sum_over(shard, axes):
        size = lax.axis_size(axes)
        spread = jnp.broadcast_to(shard[None], (size, *shard.shape))
        return jnp.sum(lax.all_to_all(spread, axes, 0, 0, tiled=True), axis=0)

    both = sum_over(jnp.sum(running, axis=2), ("row", "col"))
    mine, others = both[:, :tokens], both[:, tokens:]
    token_scores = mine + to_core(others)
    ends = jnp.cumsum(lengths)
    starts = ends - lengths

    def member(where):
        at = where * tokens + jnp.arange(tokens, dtype=jnp.int32)
        return (at[None, :] >= starts[:, None]) & (at[None, :] < ends[:, None])

    members = jnp.concatenate([member(ex_index), member(ex_index ^ 1)], axis=1)
    example_part = jnp.sum(jnp.where(members[None], both[:, None, :], 0.0), axis=2)
    example_scores = sum_over(example_part, "ex")
    return (token_scores, example_scores)


def solution(mesh):
    placed = (
        P("ex", "row"),
        P("ex", "col"),
        P("ex", "row"),
        P("ex", "col"),
        P("ex"),
        P("row", None, None),
        P("col", None, None),
        P(),
        P("row"),
        P("col"),
        P(),
    )
    return jax.shard_map(
        body, mesh=mesh, in_specs=placed, out_specs=(P(None, "ex"), P()), check_vma=False
    )
```

```python
import jax
import jax.numpy as jnp
from jax import lax
from jax.experimental import pallas as pl
from jax.experimental.pallas import tpu as pltpu
from jax.sharding import PartitionSpec as P


QUERIES = 2
DAMPING = 0.1
LANES = 128
BF = jnp.bfloat16
F32 = jnp.float32
UNREAD = pl.BlockSpec(memory_space=pl.ANY)


def vmem_limit(mib):
    return pltpu.CompilerParams(vmem_limit_bytes=mib * 2**20)


def turned_pairs(tokens, basis, pick, groups, kept, core, after=()):
    rows = tokens.shape[0]
    width = basis.shape[1]

    def kernel(core_ref, tokens_ref, basis_ref, *refs):
        step = pl.program_id(0)
        turned = jnp.dot(tokens_ref[...], basis_ref[0], preferred_element_type=F32).astype(BF)
        for group in range(groups):

            @pl.when(step // 2 == group)
            def _(group=group):
                refs[len(after) + group][0] = turned

        for n, when in enumerate(kept):

            @pl.when(step == when)
            def _(n=n):
                refs[len(after) + groups + n][...] = basis_ref[...]

    def result(group):
        return pl.BlockSpec(
            (1, rows, width), lambda n, s: (jnp.clip(n - 2 * group, 0, 1), 0, 0)
        )

    shape = jax.ShapeDtypeStruct((2, rows, width), BF)
    return pl.pallas_call(
        kernel,
        grid_spec=pltpu.PrefetchScalarGridSpec(
            num_scalar_prefetch=1,
            grid=(2 * groups,),
            in_specs=[
                pl.BlockSpec((rows, width), lambda n, s: (0, pick(n, s[0]))),
                pl.BlockSpec((1, width, width), lambda n, s: (pick(n, s[0]), 0, 0)),
            ]
            + [UNREAD] * len(after),
            out_specs=[result(group) for group in range(groups)]
            + [pl.BlockSpec((1, width, width), lambda n, s: (0, 0, 0))] * len(kept),
        ),
        out_shape=[shape] * groups
        + [jax.ShapeDtypeStruct((1, width, width), BF)] * len(kept),
        cost_estimate=pl.CostEstimate(
            flops=4 * groups * rows * width * width,
            bytes_accessed=4 * groups * (2 * rows * width + width * width),
            transcendentals=0,
        ),
        compiler_params=vmem_limit(50),
        name="turned_pairs",
    )(core[None], tokens, basis, *after)


def level_picks(levels, ref):
    row = lax.broadcasted_iota(jnp.int32, (levels, ref.shape[1]), 0)
    return jnp.where(row == ref[...], 1.0, 0.0).astype(BF)


def inverse_sides(level_table, in_levels, after=()):
    levels = level_table.shape[0]
    inputs = in_levels.shape[1]

    def kernel(table_ref, in_ref, *refs):
        table = 1.0 / (table_ref[...] + DAMPING)
        coarse = table.astype(BF)
        fine = (table - coarse.astype(F32)).astype(BF)
        chosen = level_picks(levels, in_ref)
        for n, part in enumerate((coarse, fine)):
            side = jnp.dot(part, chosen, preferred_element_type=F32)
            refs[-1][:, n * levels : (n + 1) * levels] = side.T.astype(BF)

    vmem = pl.BlockSpec(memory_space=pltpu.VMEM)
    return pl.pallas_call(
        kernel,
        in_specs=[vmem, vmem] + [UNREAD] * len(after),
        out_specs=vmem,
        out_shape=jax.ShapeDtypeStruct((inputs, 2 * levels), BF),
        compiler_params=vmem_limit(16),
        name="inverse_sides",
    )(level_table, in_levels, *after)


def gathered(pieces, split):
    rows, columns = pieces[0].shape
    count = len(pieces)

    def kernel(*refs):
        for n in range(count):
            here = slice(n * rows, (n + 1) * rows)
            refs[count][here] = refs[n][:, :split]
            refs[count + 1][here] = refs[n][:, split:]

    shapes = [(count * rows, w) for w in (split, columns - split)]
    return pl.pallas_call(
        kernel,
        grid=(1,),
        in_specs=[pl.BlockSpec((rows, columns), lambda n: (0, 0))] * count,
        out_specs=[pl.BlockSpec(shape, lambda n: (0, 0)) for shape in shapes],
        out_shape=[jax.ShapeDtypeStruct(shape, BF) for shape in shapes],
        compiler_params=vmem_limit(8),
        name="gathered",
    )(*pieces)


def parcels(query_in, query_out, query_ids, core):
    few, inner = query_in.shape
    outer = query_out.shape[1]
    width, half = inner // 2, outer // 2

    def kernel(core_ref, ids_ref, in_ref, out_ref, keep_ref, send_ref):
        row = lax.broadcasted_iota(jnp.int32, (few, LANES), 0)
        codes = jnp.zeros((few, LANES), F32)
        for n in range(few):
            codes = jnp.where(row == n, ids_ref[n].astype(F32), codes)
        codes = codes.astype(BF)

        def fill(ref, which):
            ref[:, :width] = in_ref[:, which * width : (which + 1) * width]
            ref[:, width : width + half] = out_ref[:, which * half : (which + 1) * half]
            ref[:, width + half :] = codes

        @pl.when(core_ref[0] == 0)
        def _():
            fill(keep_ref, 0)
            fill(send_ref, 1)

        @pl.when(core_ref[0] == 1)
        def _():
            fill(keep_ref, 1)
            fill(send_ref, 0)

    shape = jax.ShapeDtypeStruct((few, width + half + LANES), BF)
    smem = pl.BlockSpec(memory_space=pltpu.SMEM)
    return pl.pallas_call(
        kernel,
        grid=(1,),
        in_specs=[
            smem,
            smem,
            pl.BlockSpec((few, inner), lambda n: (0, 0)),
            pl.BlockSpec((few, outer), lambda n: (0, 0)),
        ],
        out_specs=(pl.BlockSpec(shape.shape, lambda n: (0, 0)),) * 2,
        out_shape=(shape, shape),
        compiler_params=vmem_limit(60),
        name="parcels",
    )(core[None], query_ids, query_in, query_out)


def pooled(kept, got, core, width):
    few, total = kept.shape

    def kernel(core_ref, kept_ref, got_ref, in_ref, outs_ref):
        def fill(ref, at):
            rows = slice(at, at + few)
            in_ref[rows] = ref[:, :width]
            outs_ref[rows, :width] = ref[:, width : 2 * width]
            outs_ref[rows, width : width + LANES] = ref[:, total - LANES :]
            outs_ref[rows, width + LANES :] = ref[:, 2 * width : 3 * width]

        @pl.when(core_ref[0] == 0)
        def _():
            fill(kept_ref, 0)
            fill(got_ref, few)

        @pl.when(core_ref[0] == 1)
        def _():
            fill(got_ref, 0)
            fill(kept_ref, few)

    smem = pl.BlockSpec(memory_space=pltpu.SMEM)
    shapes = [(2 * few, w) for w in (width, total - width)]
    return pl.pallas_call(
        kernel,
        grid=(1,),
        in_specs=[smem] + [pl.BlockSpec((few, total), lambda n: (0, 0))] * 2,
        out_specs=[pl.BlockSpec(shape, lambda n: (0, 0)) for shape in shapes],
        out_shape=[jax.ShapeDtypeStruct(shape, BF) for shape in shapes],
        compiler_params=vmem_limit(8),
        name="pooled",
    )(core[None], kept, got)


def rotate_turned(pieces, basis, which, after=(), strip=1024):
    rows = pieces[0].shape[0]
    width = basis.shape[1]
    count = len(pieces)

    def kernel(start_ref, *refs):
        basis_ref, out_ref = refs[count], refs[-1]
        for n in range(count):
            turned = jnp.dot(refs[n][...], basis_ref[0], preferred_element_type=F32)
            out_ref[:, n * rows : (n + 1) * rows] = turned.T.astype(BF)

    return pl.pallas_call(
        kernel,
        grid_spec=pltpu.PrefetchScalarGridSpec(
            num_scalar_prefetch=1,
            grid=(width // strip,),
            in_specs=[pl.BlockSpec((rows, width), lambda n, s: (0, 0))] * count
            + [pl.BlockSpec((1, width, strip), lambda n, s: (0, 0, n))]
            + [UNREAD] * len(after),
            out_specs=pl.BlockSpec((strip, rows * count), lambda n, s: (n, 0)),
        ),
        out_shape=jax.ShapeDtypeStruct((width, rows * count), BF),
        cost_estimate=pl.CostEstimate(
            flops=2 * count * rows * width * width,
            bytes_accessed=2 * (2 * count * rows * width + width * width),
            transcendentals=0,
        ),
        compiler_params=vmem_limit(60),
        name="rotate_turned",
    )(which[None], *pieces, basis, *after)


def spread_out(pieces, coded, basis, which, unit, after=()):
    width = basis.shape[1]
    count, rows = len(pieces), pieces[0].shape[0]
    operands = list(pieces) + ([] if pieces is coded else list(coded))

    def kernel(start_ref, *refs):
        basis_ref, out_ref = refs[len(operands)], refs[-1]
        for y in range(count):
            turned = jnp.dot(refs[y][:, :width], basis_ref[0], preferred_element_type=F32)
            codes = refs[y if pieces is coded else count + y]
            for x in range(rows // unit):
                here = slice(x * unit, (x + 1) * unit)
                code = codes[here, width : width + 1].astype(F32)
                at = (x * count + y) * unit
                for q in range(QUERIES):
                    out_ref[q, at : at + unit] = jnp.where(
                        code == float(q), turned[here], 0.0
                    ).astype(BF)

    return pl.pallas_call(
        kernel,
        grid_spec=pltpu.PrefetchScalarGridSpec(
            num_scalar_prefetch=1,
            grid=(1,),
            in_specs=[pl.BlockSpec(p.shape, lambda n, s: (0, 0)) for p in operands]
            + [pl.BlockSpec((1, width, width), lambda n, s: (0, 0, 0))]
            + [UNREAD] * len(after),
            out_specs=pl.BlockSpec((QUERIES, count * rows, width), lambda n, s: (0, 0, 0)),
        ),
        out_shape=jax.ShapeDtypeStruct((QUERIES, count * rows, width), BF),
        cost_estimate=pl.CostEstimate(
            flops=2 * count * rows * width * width,
            bytes_accessed=2 * (3 * count * rows * width + width * width),
            transcendentals=0,
        ),
        compiler_params=vmem_limit(20),
        name="spread_out",
    )(which[None], *operands, basis, *after)


def score_block(
    turned, spread, sides, out_levels, acts, grads, running, block, strip=512, rows=256
):
    width, qtokens = turned[0].shape
    parts, tokens = acts[0].shape[:2]
    total_shape = (QUERIES, 2 * tokens, LANES)
    strips = width // strip

    levels = sides.shape[1] // 2

    def kernel(t0, t1, spread_ref, sides_ref, levels_ref, far0, far1, g0, g1, *refs):
        out_ref, scratch, inverse_ref, a0, a1, semaphores = refs[-6:]
        copies = [
            pltpu.make_async_copy(far, near, semaphores.at[n])
            for n, (far, near) in enumerate(((far0, a0), (far1, a1)))
        ]

        @pl.when(pl.program_id(0) == 0)
        def _():
            for copy in copies:
                copy.start()
            out_ref[...] = jnp.zeros(total_shape, F32) if running is None else refs[0][...]

        chosen = level_picks(levels, levels_ref)
        chosen = jnp.concatenate([chosen, chosen])
        for top in range(0, parts * width, rows):
            at = slice(top, top + rows)
            inverse_ref[at] = jnp.dot(sides_ref[at], chosen, preferred_element_type=F32)

        for q in range(QUERIES):
            for p, t in enumerate((t0, t1)):
                for top in range(0, width, rows):
                    at = slice(p * width + top, p * width + top + rows)
                    piece = jnp.dot(t[top : top + rows], spread_ref[q], preferred_element_type=F32)
                    scratch[at] = (piece * inverse_ref[at]).astype(BF)
            if q == 0:

                @pl.when(pl.program_id(0) == 0)
                def _():
                    for copy in copies:
                        copy.wait()

            for side, (a, g) in enumerate(((a0, g0), (a1, g1))):
                for top in range(0, tokens, rows):
                    image = None
                    for p in range(parts):
                        term = jnp.dot(
                            a[p if side == 0 else 1 - p, top : top + rows],
                            scratch[p * width : (p + 1) * width],
                            preferred_element_type=F32,
                        )
                        image = term if image is None else image + term
                    terms = image * g[0, top : top + rows].astype(F32)
                    total = terms[:, :LANES]
                    for lane in range(LANES, strip, LANES):
                        total = total + terms[:, lane : lane + LANES]
                    at = side * tokens + top
                    out_ref[q, at : at + rows] += total

    once = pl.Buffered(1)
    whole = pl.BlockSpec(memory_space=pltpu.HBM)
    turned_spec = pl.BlockSpec((width, qtokens), lambda n: (0, 0), pipeline_mode=once)
    strip_spec = pl.BlockSpec((1, tokens, strip), lambda n: (block, 0, n))
    run_spec = pl.BlockSpec(total_shape, lambda n: (0, 0, 0), pipeline_mode=once)
    flops = 2 * QUERIES * parts * width * width * (qtokens + 2 * tokens)
    return pl.pallas_call(
        kernel,
        grid=(strips,),
        in_specs=[
            turned_spec,
            turned_spec,
            pl.BlockSpec((QUERIES, qtokens, strip), lambda n: (0, 0, n)),
            pl.BlockSpec(sides.shape, lambda n: (0, 0), pipeline_mode=once),
            pl.BlockSpec((1, strip), lambda n: (0, block * strips + n)),
            whole,
            whole,
            strip_spec,
            strip_spec,
        ]
        + ([] if running is None else [run_spec]),
        out_specs=pl.BlockSpec(total_shape, lambda n: (0, 0, 0)),
        out_shape=jax.ShapeDtypeStruct(total_shape, F32),
        scratch_shapes=[
            pltpu.VMEM((parts * width, strip), BF),
            pltpu.VMEM((parts * width, strip), F32),
            pltpu.VMEM(acts[0].shape, BF),
            pltpu.VMEM(acts[0].shape, BF),
            pltpu.SemaphoreType.DMA((2,)),
        ],
        cost_estimate=pl.CostEstimate(flops=flops, bytes_accessed=16 * 2**20, transcendentals=0),
        compiler_params=vmem_limit(32),
        name="score_block",
    )(*turned, spread, sides, out_levels, *acts, *grads, *([] if running is None else [running]))


def body(
    train_in,
    train_out,
    query_in,
    query_out,
    query_ids,
    in_basis,
    out_basis,
    level_table,
    in_level,
    out_level,
    lengths,
):
    ex_count = lax.axis_size("ex")
    ex_index = lax.axis_index("ex")
    core = ex_index % 2
    in_sub, width = in_basis.shape[0], in_basis.shape[1]
    out_sub = out_basis.shape[0]
    half = out_sub // 2
    tokens = train_in.shape[0]
    few = query_in.shape[0]
    hops = ex_count // 4

    def to_core(a):
        return lax.ppermute(a, "ex", [(i, i ^ 1) for i in range(ex_count)])

    def across_y(a):
        return lax.ppermute(a, "ex", [(i, i ^ 2) for i in range(ex_count)])

    def across_y_and_col(a):
        count = lax.axis_size("col") * ex_count
        return lax.ppermute(a, ("col", "ex"), [(i, i ^ ex_count ^ 2) for i in range(count)])

    def along_x(a):
        result = [a]
        for n in range(1, hops):
            pairs = [(i, (i + 4 * n) % ex_count) for i in range(ex_count)]
            result.append(lax.ppermute(a, "ex", pairs))
        return result

    kept, sent = parcels(query_in, query_out, query_ids, core)
    near_in, near_out = pooled(kept, to_core(sent), core, width)
    near_in_y = across_y_and_col(near_in)
    column = jnp.concatenate([near_in, near_in_y])
    row = along_x(near_out)
    rows = gathered(row, width + LANES)
    grads_away, grads_own, *outers = turned_pairs(
        train_out,
        out_basis,
        lambda n, c: jnp.where(n < 2, (1 - c) * 2 + n, c * 2 + n - 2),
        2,
        (2, 3),
        core,
        (near_in,),
    )
    grads_other = to_core(grads_away)
    in_pieces = along_x(column)
    first_pieces = [rows[0], across_y(rows[0])]
    second_pieces = [rows[1], across_y(rows[1])]
    acts_own, inner = turned_pairs(
        train_in,
        in_basis,
        lambda n, c: jnp.where(n < 1, c, 1 - c),
        1,
        (0,),
        core,
        (column, *rows),
    )
    acts_other = to_core(acts_own)

    in_levels = in_level.reshape(in_sub, width)
    in_levels = jnp.concatenate(
        [lax.dynamic_slice_in_dim(in_levels, n, 1) for n in (core, 1 - core)], axis=1
    )
    out_levels = lax.dynamic_slice_in_dim(out_level, core * half * width, half * width)[None]
    sides = inverse_sides(level_table, in_levels)

    query_own = rotate_turned(in_pieces, inner, core)
    query_other = to_core(query_own)
    running = None
    for block, pieces in enumerate((first_pieces, second_pieces)):
        spread = spread_out(
            pieces,
            first_pieces,
            outers[block],
            core,
            2 * few,
            () if running is None else (running,),
        )
        running = score_block(
            (query_own, query_other),
            spread,
            sides,
            out_levels,
            (acts_own, acts_other),
            (grads_own, grads_other),
            running,
            block,
        )

    def sum_over(shard, axes):
        size = lax.axis_size(axes)
        spread = jnp.broadcast_to(shard[None], (size, *shard.shape))
        return jnp.sum(lax.all_to_all(spread, axes, 0, 0, tiled=True), axis=0)

    both = sum_over(jnp.sum(running, axis=2), ("row", "col"))
    mine, others = both[:, :tokens], both[:, tokens:]
    token_scores = mine + to_core(others)
    ends = jnp.cumsum(lengths)
    starts = ends - lengths

    def member(where):
        at = where * tokens + jnp.arange(tokens, dtype=jnp.int32)
        return (at[None, :] >= starts[:, None]) & (at[None, :] < ends[:, None])

    members = jnp.concatenate([member(ex_index), member(ex_index ^ 1)], axis=1)
    example_part = jnp.sum(jnp.where(members[None], both[:, None, :], 0.0), axis=2)
    example_scores = sum_over(example_part, "ex")
    return (token_scores, example_scores)


def solution(mesh):
    placed = (
        P("ex", "row"),
        P("ex", "col"),
        P("ex", "row"),
        P("ex", "col"),
        P("ex"),
        P("row", None, None),
        P("col", None, None),
        P(),
        P("row"),
        P("col"),
        P(),
    )
    return jax.shard_map(
        body, mesh=mesh, in_specs=placed, out_specs=(P(None, "ex"), P()), check_vma=False
    )
```
